32 devices in a mesh: lang: 8 (over z, core), shard: 4 (over y, x).
Axes of the slice: x: 2, y: 2, z: 4, core: 2. Of those that a mesh axis runs over, the one named last changes fastest.
Arguments:
- queries: bfloat16 [4096, 768], P(('lang', 'shard')), may hold values from -6 to 6
- routes: int32 [4096, 1], P(('lang', 'shard')), may hold values from 0 to 7; in each aligned block of 128 rows (0 to 127, 128 to 255, ...) at most 20 rows name the same one
- corpus: bfloat16 [32768, 768], P(('lang', 'shard')), may hold values from -0.21875 to 0.21875
Outputs:
- top_scores: float32 [4096, 128], P(('lang', 'shard'))
The draws below stay inside these ranges and needn't reach their ends.
Inputs may be any that keep to these rules, and one draw needn't show every extreme that they name: `routes`: among the 128 queries of one device, each language is named at most 20 times; some language is named exactly 20 times.
All inputs are finite; a program needn't handle non-finite values.
Results may differ from the reference program's by a relative error of at most 0.0012.
Values may be sent and summed in bfloat16 or wider, within the bound.
A program may use at most 64 MiB of HBM per device.

```python
import math
import jax
import jax.numpy as jnp
import numpy as np
from jax import lax

D = 768
Q_DEV = 128
PASS_DEV = 1024
CAP = 20
TOPK = 128
QUERIES = 4096
PASSAGES = 32768
N_LANG = 8
N_SHARD = 4


def block_levels(rng, extent, cuts, least, largest):
    def one(dim, shards_of):
        steps = jax.random.uniform(jax.random.fold_in(jax.random.fold_in(rng, 6), dim), (shards_of,), jnp.float32, least / len(cuts), largest / len(cuts))
        return jnp.repeat(jnp.exp(steps), extent[dim] // shards_of).reshape((-1,) + (1,) * (len(extent) - dim - 1))

    gain = one(*cuts[0])
    for cut in cuts[1:]:
        gain = gain * one(*cut)
    return gain


def deal_out(own_key, own, number, rows, count, top, most, slope):
    order = jax.random.permutation(own_key, count)
    heavy_load, ordinary = portions_of(count, rows * top, most, slope, True), portions_of(count, rows * top, most, slope, False)
    places = jnp.arange(count)

    def named(tallies, turn):
        used = int((tallies > 0).sum())
        fixed = max(1, used // 4)
        shifted = fixed + (places - fixed + turn * (used - fixed)) % max(1, count - fixed)
        return jnp.zeros((count,), jnp.int32).at[order[jnp.where(places < fixed, places, shifted)]].set(jnp.asarray(tallies, jnp.int32))

    tallies = jnp.where(number % 4 == 0, named(heavy_load, number // 4), named(ordinary, number - number // 4 - 1))
    mixed = jax.random.permutation(jax.random.fold_in(own, 3), count)
    giver, sink = mixed[0:count // 2 * 2:2], mixed[1:count // 2 * 2:2]
    margin = jnp.minimum(tallies[giver] - 1, most - tallies[sink]) // 2
    margin = jnp.where((giver == order[0]) | (sink == order[0]) | (tallies[sink] == 0), 0, jnp.maximum(margin, 0))
    shifted = jax.random.randint(jax.random.fold_in(own, 4), (count // 2,), 0, 1 << 20) % (margin + 1)
    tallies = tallies.at[giver].add(-shifted).at[sink].add(shifted)
    items = jnp.searchsorted(jnp.cumsum(tallies), jnp.arange(rows * top), side="right").astype(jnp.int32)
    grid = items.reshape(top, rows).T
    grid = grid[jax.random.permutation(jax.random.fold_in(own, 1), rows)]
    turn = jax.random.randint(jax.random.fold_in(own, 2), (rows, 1), 0, top)
    return jnp.take_along_axis(grid, (jnp.arange(top)[None, :] + turn) % top, axis=1)


def portions_of(number_of, total, bound, lean, full):
    weights = [(1 << 20) // math.isqrt(standing ** lean) + 1 for standing in range(1, number_of + 1)]
    largest = bound if full else min(bound, max(-(-total // number_of), total * weights[0] // sum(weights)))
    least = 1 if total - largest >= number_of - 1 else 0
    holding, surplus = [largest] + [least] * (number_of - 1), total - largest - least * (number_of - 1)
    while surplus > 0:
        movable = [i for i in range(1, number_of) if holding[i] < largest] or [i for i in range(1, number_of) if holding[i] < bound]
        mass, left = sum([weights[i] for i in movable]), surplus
        for i in movable:
            extra = min(bound - holding[i], max(1, left * weights[i] // mass), surplus)
            holding[i] = holding[i] + extra
            surplus = surplus - extra
    return np.array(holding)


def gaussian(rng, shape, deviation, reach, shards=(), held_as=jnp.bfloat16):
    drawn = deviation * jax.random.normal(rng, shape, jnp.float32)
    if shards:
        drawn = drawn * block_levels(rng, shape, shards, -0.22, 0.18)
    return jnp.clip(drawn, -reach, reach).astype(held_as)


def setup_inputs(seed: int = 0) -> dict:
    arg_keys = jax.random.split(jax.random.key(seed), 4)
    queries = gaussian(arg_keys[0], (QUERIES, D), 1.0, 6.0, ((0, 32),))
    routes_keys = jax.random.split(jax.random.fold_in(arg_keys[1], 1), QUERIES // Q_DEV)
    routes_turns = jax.random.permutation(jax.random.fold_in(arg_keys[1], 3), QUERIES // Q_DEV)
    routes = jax.vmap(lambda own, number: deal_out(jax.random.fold_in(arg_keys[1], 2), own, number, Q_DEV, N_LANG, 1, CAP, 2))(routes_keys, routes_turns).reshape((QUERIES, 1))
    corpus = gaussian(arg_keys[2], (PASSAGES, D), D ** -0.5, 0.21875, ((0, 32),))
    return dict(queries=queries, routes=routes, corpus=corpus)


epsilon = 1e-06

def reference(queries, routes, corpus):
    widened = queries.astype(jnp.float32)
    unit_query = (widened * lax.rsqrt(lax.optimization_barrier(jnp.mean(widened * widened, axis=1, keepdims=True)) + epsilon)).astype(jnp.bfloat16)
    devices_count = N_LANG * N_SHARD
    language = routes[:, 0].reshape(devices_count, Q_DEV).astype(jnp.int32)
    onehot = (language[:, :, None] == jnp.arange(N_LANG, dtype=jnp.int32)[None, None, :]).astype(jnp.int32)
    slot_index = (lax.optimization_barrier(jnp.sum(jnp.cumsum(onehot, axis=1) * onehot, axis=2)) - 1).astype(jnp.int32)
    device_index = jnp.broadcast_to(jnp.arange(devices_count, dtype=jnp.int32)[:, None], (devices_count, Q_DEV))
    padded = jnp.zeros((devices_count, N_LANG, CAP, D), jnp.bfloat16)
    padded = padded.at[device_index, language, slot_index].set(unit_query.reshape(devices_count, Q_DEV, D))
    blocks = jnp.transpose(padded, (1, 0, 2, 3)).reshape(N_LANG, devices_count * CAP, D)
    lang_corpus = corpus.reshape(N_LANG, N_SHARD * PASS_DEV, D)

    def score_language(inputs):
        block_rows, passages = inputs
        scores = jnp.dot(block_rows.astype(jnp.float32), passages.astype(jnp.float32).T, precision=lax.Precision.HIGHEST)
        return lax.top_k(scores, TOPK)[0]
    results = lax.map(score_language, (blocks, lang_corpus))
    results = results.reshape(N_LANG, devices_count, CAP, TOPK)
    picked = results[language, device_index, slot_index]
    return picked.reshape(devices_count * Q_DEV, TOPK)
```

```python
import functools
import jax
import jax.numpy as jnp
from jax import lax
from jax.experimental import pallas as pl
from jax.experimental.pallas import tpu as pltpu
from jax.sharding import PartitionSpec as P

CAP = 20
TOPK = 128
LANES = 128
SUB = 8
PART = 32


epsilon = 1e-06


def exchange(values, i, j):
    values[i], values[j] = jnp.maximum(values[i], values[j]), jnp.minimum(values[i], values[j])


def sort_down(values):
    values = list(values)
    n = len(values)
    p = 1
    while p < n:
        k = p
        while k >= 1:
            for j in range(k % p, n - k, 2 * k):
                for i in range(min(k, n - j - k)):
                    if (i + j) // (2 * p) == (i + j + k) // (2 * p):
                        exchange(values, i + j, i + j + k)
            k //= 2
        p *= 2
    return values


def bitonic_down(values):
    values = list(values)
    d = len(values) // 2
    while d:
        for i in range(len(values)):
            if not i & d:
                exchange(values, i, i + d)
        d //= 2
    return values


def top_block(x, y, put):
    n = TOPK
    for g in range(n // PART):
        run = sort_down([x[g * PART + i] for i in range(PART)])
        for i in range(PART):
            x[g * PART + (i if g % 2 == 0 else PART - 1 - i)] = run[i]
    for g in range(2):
        base = g * 2 * PART
        for half, take in enumerate((jnp.maximum, jnp.minimum)):
            run = bitonic_down([take(x[base + i], x[base + PART + i]) for i in range(PART)])
            for i in range(PART):
                at = half * PART + i
                y[base + (at if g == 0 else 2 * PART - 1 - at)] = run[i]

    def quarters(source, target, pick):
        for i in range(PART):
            four = [pick(source, i + PART * j) for j in range(4)]
            four = bitonic_down(four)
            for j in range(4):
                target[i + PART * j] = four[j]

    def finish(source, store):
        for g in range(4):
            run = bitonic_down([source[g * PART + i] for i in range(PART)])
            for i in range(PART):
                store(g * PART + i, run[i])

    def keep(target):
        def store(i, v):
            target[i] = v
        return store

    quarters(y, x, lambda s, i: s[i])
    finish(x, keep(y))
    source, target = y, x
    for shift in (4, 2, 1):
        quarters(
            source, target,
            lambda s, i: jnp.maximum(s[i], pltpu.roll(s[n - 1 - i], shift, 0)),
        )
        finish(target, put if shift == 1 else keep(source))


def top_kernel(q_ref, c_ref, o_ref, x, y, t):
    blocks = q_ref.shape[0] // LANES

    def put(i, v):
        t[pl.ds(i, 1), :] = v[i % SUB:i % SUB + 1, :]

    def step(b, carry):
        rows = pl.ds(pl.multiple_of(b * LANES, LANES), LANES)
        scores = lax.dot_general(
            c_ref[...], q_ref[rows, :], (((1,), (1,)), ((), ())),
            preferred_element_type=jnp.float32,
        )
        x[...] = scores.reshape(x.shape)
        top_block(x, y, put)
        o_ref[rows, :] = t[...].T
        return carry

    lax.fori_loop(0, blocks, step, 0)


def score_block(query_rows, corpus):
    count = query_rows.shape[0]
    return pl.pallas_call(
        top_kernel,
        out_shape=jax.ShapeDtypeStruct((count, TOPK), jnp.float32),
        in_specs=[pl.BlockSpec(memory_space=pltpu.VMEM)] * 2,
        out_specs=pl.BlockSpec(memory_space=pltpu.VMEM),
        scratch_shapes=[pltpu.VMEM((TOPK, SUB, LANES), jnp.float32)] * 2
        + [pltpu.VMEM((TOPK, LANES), jnp.float32)],
    )(query_rows, corpus)


def shards(queries, routes, corpus):
    lang_count = lax.axis_size("lang")
    feature_count = queries.shape[1]
    capacity = CAP
    keep_count = TOPK
    widened = queries.astype(jnp.float32)
    unit_query = (
        widened * lax.rsqrt(jnp.mean(widened * widened, axis=1, keepdims=True) + epsilon)
    ).astype(jnp.bfloat16)
    language = routes[:, 0]
    onehot = (language[:, None] == jnp.arange(lang_count, dtype=jnp.int32)[None, :]).astype(
        jnp.int32
    )
    slot_index = jnp.sum(jnp.cumsum(onehot, axis=0) * onehot, axis=1) - 1
    position = language * capacity + slot_index
    outbox = (
        jnp.zeros((lang_count * capacity, feature_count), jnp.bfloat16).at[position].set(unit_query)
    )
    arrived = lax.all_to_all(outbox, "lang", split_axis=0, concat_axis=0, tiled=True)
    candidates = score_block(
        lax.all_gather(arrived, "shard", axis=0, tiled=True), corpus
    )
    pooled = lax.all_to_all(candidates, "shard", split_axis=0, concat_axis=1, tiled=True)
    owned = lax.top_k(pooled, keep_count)[0]
    returned = lax.all_to_all(owned, "lang", split_axis=0, concat_axis=0, tiled=True)
    return returned[position]


def solution(mesh):
    placed = (P(("lang", "shard"), None), P(("lang", "shard"), None), P(("lang", "shard"), None))
    return jax.shard_map(
        shards, mesh=mesh, in_specs=placed, out_specs=P(("lang", "shard"), None), check_vma=False
    )
```

```python
import functools
import jax
import jax.numpy as jnp
from jax import lax
from jax.experimental import pallas as pl
from jax.experimental.pallas import tpu as pltpu
from jax.sharding import PartitionSpec as P

CAP = 20
TOPK = 128
LANES = 128
SUB = 8
PART = 32
BACK = 24
SENT = 32
MESH = pl.DeviceIdType.MESH


epsilon = 1e-06


def exchange(values, i, j):
    values[i], values[j] = jnp.maximum(values[i], values[j]), jnp.minimum(values[i], values[j])


def sort_down(values):
    values = list(values)
    n = len(values)
    p = 1
    while p < n:
        k = p
        while k >= 1:
            for j in range(k % p, n - k, 2 * k):
                for i in range(min(k, n - j - k)):
                    if (i + j) // (2 * p) == (i + j + k) // (2 * p):
                        exchange(values, i + j, i + j + k)
            k //= 2
        p *= 2
    return values


def bitonic_down(values):
    values = list(values)
    d = len(values) // 2
    while d:
        for i in range(len(values)):
            if not i & d:
                exchange(values, i, i + d)
        d //= 2
    return values


def top_block(x, y, put, sign):
    n = TOPK
    for g in range(n // PART):
        run = sort_down([x[g * PART + i] for i in range(PART)])
        for i in range(PART):
            x[g * PART + (i if g % 2 == 0 else PART - 1 - i)] = run[i]
    for g in range(2):
        base = g * 2 * PART
        for half, take in enumerate((jnp.maximum, jnp.minimum)):
            run = bitonic_down([take(x[base + i], x[base + PART + i]) for i in range(PART)])
            for i in range(PART):
                at = half * PART + i
                y[base + (at if g == 0 else 2 * PART - 1 - at)] = run[i]

    def quarters(source, target, pick):
        for i in range(PART):
            four = [pick(source, i + PART * j) for j in range(4)]
            four = bitonic_down(four)
            for j in range(4):
                target[i + PART * j] = four[j]

    def finish(source, store):
        for g in range(4):
            run = bitonic_down([source[g * PART + i] for i in range(PART)])
            for i in range(PART):
                store(g * PART + i, run[i])

    def keep(target):
        def store(i, v):
            target[i] = v
        return store

    quarters(y, x, lambda s, i: s[i])
    finish(x, keep(y))
    source, target = y, x
    for shift in (4, 2, 1):
        def pick(s, i, shift=shift):
            best = jnp.maximum(s[i], pltpu.roll(s[n - 1 - i], shift, 0))
            return best * sign if shift == 1 else best

        quarters(source, target, pick)
        finish(target, put if shift == 1 else keep(source))


def merge_lanes(values, down):
    lane = lax.broadcasted_iota(jnp.int32, values.shape, 1)
    d = LANES // 2
    while d:
        above = pltpu.roll(values, LANES - d, 1)
        below = pltpu.roll(values, d, 1)
        low = (lane & d) == 0
        if down:
            values = jnp.where(low, jnp.maximum(values, above), jnp.minimum(values, below))
        else:
            values = jnp.where(low, jnp.minimum(values, above), jnp.maximum(values, below))
        d //= 2
    return values


def place(shape, slots):
    return (lax.broadcasted_iota(jnp.int32, shape, 0) == slots).astype(jnp.float32)


def kernel(
    langs, shard_count, q_ref, r_ref, c_hbm, o_ref,
    corpus, outbox, inbox, gathered, x, y, t, result, cand, merged, ret, back, unroute,
    c_sem, a_send, a_recv, b_send, b_recv, r_send, r_recv, z_send, z_recv,
):
    my_lang = lax.axis_index("lang")
    my_shard = lax.axis_index("shard")
    rows = langs * CAP
    part = LANES // shard_count
    chunks = rows // part

    load = pltpu.make_async_copy(c_hbm, corpus, c_sem)
    load.start()

    barrier = pltpu.get_barrier_semaphore()
    for step in range(1, langs):
        pl.semaphore_signal(
            barrier, inc=1, device_id=(lax.rem(my_lang + step, langs), my_shard), device_id_type=MESH
        )
    for step in range(1, shard_count):
        pl.semaphore_signal(
            barrier, inc=1, device_id=(my_lang, lax.rem(my_shard + step, shard_count)),
            device_id_type=MESH,
        )

    widened = q_ref[...].astype(jnp.float32)
    unit = (
        widened * lax.rsqrt(jnp.mean(widened * widened, axis=1, keepdims=True) + epsilon)
    ).astype(jnp.bfloat16)
    count = q_ref.shape[0]
    language = r_ref[...]
    onehot = (lax.broadcasted_iota(jnp.int32, (langs, count), 0) == language).astype(jnp.float32)
    upto = (
        lax.broadcasted_iota(jnp.int32, (count, count), 0)
        <= lax.broadcasted_iota(jnp.int32, (count, count), 1)
    ).astype(jnp.bfloat16)
    ranks = jnp.dot(onehot.astype(jnp.bfloat16), upto, preferred_element_type=jnp.float32)
    slot = jnp.sum(ranks * onehot, axis=0, keepdims=True).astype(jnp.int32) - 1
    sends = place((langs * SENT, count), language * SENT + slot).astype(jnp.bfloat16)
    outbox[...] = (
        jnp.dot(sends, unit, preferred_element_type=jnp.float32)
        .astype(jnp.bfloat16)
        .reshape(outbox.shape)
    )
    pl.semaphore_wait(barrier, langs - 1 + shard_count - 1)

    def over_lang(source, target, send_sems, recv_sems, step):
        to = lax.rem(my_lang + step, langs)
        return pltpu.make_async_remote_copy(
            src_ref=source.at[to], dst_ref=target.at[my_lang],
            send_sem=send_sems.at[to], recv_sem=recv_sems.at[my_lang],
            device_id=(to, my_shard), device_id_type=MESH,
        )

    def from_lang(source, target, send_sems, recv_sems, step):
        origin = lax.rem(my_lang + langs - step, langs)
        return pltpu.make_async_remote_copy(
            src_ref=source.at[origin], dst_ref=target.at[origin],
            send_sem=send_sems.at[origin], recv_sem=recv_sems.at[origin],
            device_id=(origin, my_shard), device_id_type=MESH,
        )

    for step in range(1, langs):
        over_lang(outbox, inbox, a_send, a_recv, step).start()
    inbox[my_lang] = outbox[my_lang]

    unroute[...] = place((langs * BACK, count), language * BACK + slot).T
    ret[...] = jnp.zeros_like(ret)
    row = lax.broadcasted_iota(jnp.int32, (rows, langs * SENT), 0)
    compact = (
        lax.broadcasted_iota(jnp.int32, (rows, langs * SENT), 1) == row // CAP * SENT + row % CAP
    ).astype(jnp.bfloat16)

    for step in range(1, langs):
        from_lang(outbox, inbox, a_send, a_recv, step).wait_recv()
    gathered[my_shard] = jnp.dot(
        compact, inbox[...].reshape(langs * SENT, -1), preferred_element_type=jnp.float32
    ).astype(jnp.bfloat16)

    def piece(c):
        return pl.ds(pl.multiple_of(c * part, part), part)

    def over_shard(c, step):
        to = lax.rem(my_shard + step, shard_count)
        return pltpu.make_async_remote_copy(
            src_ref=gathered.at[my_shard, piece(c)], dst_ref=gathered.at[my_shard, piece(c)],
            send_sem=b_send.at[to, c], recv_sem=b_recv.at[my_shard, c],
            device_id=(my_lang, to), device_id_type=MESH,
        )

    def from_shard(c, step):
        origin = lax.rem(my_shard + shard_count - step, shard_count)
        return pltpu.make_async_remote_copy(
            src_ref=gathered.at[origin, piece(c)], dst_ref=gathered.at[origin, piece(c)],
            send_sem=b_send.at[origin, c], recv_sem=b_recv.at[origin, c],
            device_id=(my_lang, origin), device_id_type=MESH,
        )

    def answer(c, step):
        to = lax.rem(my_shard + step, shard_count)
        return pltpu.make_async_remote_copy(
            src_ref=result.at[c, to], dst_ref=cand.at[my_shard, piece(c)],
            send_sem=r_send.at[to, c], recv_sem=r_recv.at[my_shard, c],
            device_id=(my_lang, to), device_id_type=MESH,
        )

    def answered(c, step):
        origin = lax.rem(my_shard + shard_count - step, shard_count)
        return pltpu.make_async_remote_copy(
            src_ref=result.at[c, origin], dst_ref=cand.at[origin, piece(c)],
            send_sem=r_send.at[origin, c], recv_sem=r_recv.at[origin, c],
            device_id=(my_lang, origin), device_id_type=MESH,
        )

    def send_pieces(c, carry):
        for step in range(1, shard_count):
            over_shard(c, step).start()
        return carry

    lax.fori_loop(0, chunks, send_pieces, 0)
    load.wait()
    sign = (1 - 2 * lax.rem(my_shard, 2)).astype(jnp.float32)

    def put(i, v):
        t[pl.ds(i, 1), :] = v[i % SUB:i % SUB + 1, :]

    def score(c, carry):
        for step in range(1, shard_count):
            from_shard(c, step).wait_recv()
        block = jnp.concatenate([gathered[s, piece(c)] for s in range(shard_count)], axis=0)
        scores = lax.dot_general(
            corpus[...], block, (((1,), (1,)), ((), ())), preferred_element_type=jnp.float32
        )
        x[...] = scores.reshape(x.shape)
        top_block(x, y, put, sign)
        result[c] = (t[...] * sign).T.reshape(shard_count, part, TOPK)
        for step in range(1, shard_count):
            answer(c, step).start()
        cand[my_shard, piece(c)] = result[c, my_shard]
        return carry

    lax.fori_loop(0, chunks, score, 0)

    def settle(c, carry):
        for step in range(1, shard_count):
            answered(c, step).wait_recv()
        return carry

    lax.fori_loop(0, chunks, settle, 0)
    lists = [cand[s] for s in range(shard_count)]
    while len(lists) > 1:
        lists = [
            merge_lanes(jnp.maximum(lists[2 * k], lists[2 * k + 1]), k % 2 == 0)
            for k in range(len(lists) // 2)
        ]
    merged[...] = lists[0]
    for l in range(langs):
        ret[l, 0:CAP, :] = merged[l * CAP:(l + 1) * CAP, :]
    for step in range(1, langs):
        over_lang(ret, back, z_send, z_recv, step).start()
    back[my_lang] = ret[my_lang]

    def drain(c, carry):
        for step in range(1, shard_count):
            over_shard(c, step).wait_send()
            answer(c, step).wait_send()
        return carry

    lax.fori_loop(0, chunks, drain, 0)
    for step in range(1, langs):
        over_lang(outbox, inbox, a_send, a_recv, step).wait_send()
    for step in range(1, langs):
        from_lang(ret, back, z_send, z_recv, step).wait_recv()
    o_ref[...] = jnp.dot(
        unroute[...], back[...].reshape(langs * BACK, TOPK),
        preferred_element_type=jnp.float32, precision=lax.Precision.HIGHEST,
    )
    for step in range(1, langs):
        over_lang(ret, back, z_send, z_recv, step).wait_send()


def shards(queries, routes, corpus):
    langs = lax.axis_size("lang")
    shard_count = lax.axis_size("shard")
    count, features = queries.shape
    rows = langs * CAP
    part = LANES // shard_count
    chunks = rows // part
    dma = pltpu.SemaphoreType.DMA
    per_piece = [dma((shard_count, chunks))] * 4
    f32, bf16 = jnp.float32, jnp.bfloat16
    return pl.pallas_call(
        functools.partial(kernel, langs, shard_count),
        out_shape=jax.ShapeDtypeStruct((count, TOPK), f32),
        in_specs=[
            pl.BlockSpec(memory_space=pltpu.VMEM),
            pl.BlockSpec(memory_space=pltpu.VMEM),
            pl.BlockSpec(memory_space=pl.ANY),
        ],
        out_specs=pl.BlockSpec(memory_space=pltpu.VMEM),
        scratch_shapes=[
            pltpu.VMEM(corpus.shape, bf16),
            pltpu.VMEM((langs, SENT, features), bf16),
            pltpu.VMEM((langs, SENT, features), bf16),
            pltpu.VMEM((shard_count, rows, features), bf16),
            pltpu.VMEM((TOPK, SUB, LANES), f32),
            pltpu.VMEM((TOPK, SUB, LANES), f32),
            pltpu.VMEM((TOPK, LANES), f32),
            pltpu.VMEM((chunks, shard_count, part, TOPK), f32),
            pltpu.VMEM((shard_count, rows, TOPK), f32),
            pltpu.VMEM((rows, TOPK), f32),
            pltpu.VMEM((langs, BACK, TOPK), f32),
            pltpu.VMEM((langs, BACK, TOPK), f32),
            pltpu.VMEM((count, langs * BACK), f32),
            dma, dma((langs,)), dma((langs,)), *per_piece, dma((langs,)), dma((langs,)),
        ],
        compiler_params=pltpu.CompilerParams(collective_id=0, has_side_effects=True),
    )(queries, routes.reshape(1, count), corpus)


def solution(mesh):
    placed = (P(("lang", "shard"), None), P(("lang", "shard"), None), P(("lang", "shard"), None))
    return jax.shard_map(
        shards, mesh=mesh, in_specs=placed, out_specs=P(("lang", "shard"), None), check_vma=False
    )
```

```python
import functools
import jax
import jax.numpy as jnp
from jax import lax
from jax.experimental import pallas as pl
from jax.experimental.pallas import tpu as pltpu
from jax.sharding import PartitionSpec as P

CAP = 20
TOPK = 128
LANES = 128
SUB = 8
PART = 32
MAIN = 16
REST = CAP - MAIN
PACK = 32
TAIL = 8
MESH = pl.DeviceIdType.MESH


epsilon = 1e-06


def exchange(values, i, j):
    values[i], values[j] = jnp.maximum(values[i], values[j]), jnp.minimum(values[i], values[j])


def sort_down(values):
    values = list(values)
    n = len(values)
    p = 1
    while p < n:
        k = p
        while k >= 1:
            for j in range(k % p, n - k, 2 * k):
                for i in range(min(k, n - j - k)):
                    if (i + j) // (2 * p) == (i + j + k) // (2 * p):
                        exchange(values, i + j, i + j + k)
            k //= 2
        p *= 2
    return values


def bitonic_down(values):
    values = list(values)
    d = len(values) // 2
    while d:
        for i in range(len(values)):
            if not i & d:
                exchange(values, i, i + d)
        d //= 2
    return values


def top_block(x, y, put, sign):
    n = TOPK
    for g in range(n // PART):
        run = sort_down([x[g * PART + i] for i in range(PART)])
        for i in range(PART):
            x[g * PART + (i if g % 2 == 0 else PART - 1 - i)] = run[i]
    for g in range(2):
        base = g * 2 * PART
        for half, take in enumerate((jnp.maximum, jnp.minimum)):
            run = bitonic_down([take(x[base + i], x[base + PART + i]) for i in range(PART)])
            for i in range(PART):
                at = half * PART + i
                y[base + (at if g == 0 else 2 * PART - 1 - at)] = run[i]

    def quarters(source, target, pick):
        for i in range(PART):
            four = [pick(source, i + PART * j) for j in range(4)]
            four = bitonic_down(four)
            for j in range(4):
                target[i + PART * j] = four[j]

    def finish(source, store):
        for g in range(4):
            run = bitonic_down([source[g * PART + i] for i in range(PART)])
            for i in range(PART):
                store(g * PART + i, run[i])

    def keep(target):
        def store(i, v):
            target[i] = v
        return store

    quarters(y, x, lambda s, i: s[i])
    finish(x, keep(y))
    source, target = y, x
    for shift in (4, 2, 1):
        def pick(s, i, shift=shift):
            best = jnp.maximum(s[i], pltpu.roll(s[n - 1 - i], shift, 0))
            return best * sign if shift == 1 else best

        quarters(source, target, pick)
        finish(target, put if shift == 1 else keep(source))


def merge_lanes(values, down):
    lane = lax.broadcasted_iota(jnp.int32, values.shape, 1)
    d = LANES // 2
    while d:
        above = pltpu.roll(values, LANES - d, 1)
        below = pltpu.roll(values, d, 1)
        low = (lane & d) == 0
        if down:
            values = jnp.where(low, jnp.maximum(values, above), jnp.minimum(values, below))
        else:
            values = jnp.where(low, jnp.minimum(values, above), jnp.maximum(values, below))
        d //= 2
    return values


def place(shape, slots):
    return (lax.broadcasted_iota(jnp.int32, shape, 0) == slots).astype(jnp.float32)


def kernel(
    langs, shard_count, q_ref, r_ref, c_hbm, o_ref,
    corpus, out_main, out_rest, all_main, all_rest, block, x, y, t, result, cand,
    ret_main, ret_rest, back_main, back_rest, un_main, un_rest,
    c_sem, am_send, am_recv, ar_send, ar_recv, bm_send, bm_recv, br_send, br_recv,
    r_send, r_recv, zm_send, zm_recv, zr_send, zr_recv,
):
    my_lang = lax.axis_index("lang")
    my_shard = lax.axis_index("shard")
    group = LANES // MAIN // shard_count
    groups = langs // group
    tails = langs * REST * shard_count // LANES
    tail_langs = langs // tails
    part = LANES // shard_count
    chunks = groups + tails
    my_group, my_place = my_lang // group, lax.rem(my_lang, group)
    steps = [(d, k) for d in range(groups) for k in range(group) if d or k]

    load = pltpu.make_async_copy(c_hbm, corpus, c_sem)
    load.start()

    def later(d, k):
        return lax.rem(my_group + d, groups) * group + lax.rem(my_place + k, group)

    def earlier(d, k):
        return lax.rem(my_group + groups - d, groups) * group + lax.rem(my_place + group - k, group)

    def next_shard(step):
        return lax.rem(my_shard + step, shard_count)

    def last_shard(step):
        return lax.rem(my_shard + shard_count - step, shard_count)

    barrier = pltpu.get_barrier_semaphore()
    for d, k in steps:
        pl.semaphore_signal(barrier, inc=1, device_id=(later(d, k), my_shard), device_id_type=MESH)
    for step in range(1, shard_count):
        pl.semaphore_signal(
            barrier, inc=1, device_id=(my_lang, next_shard(step)), device_id_type=MESH
        )

    widened = q_ref[...].astype(jnp.float32)
    unit = (
        widened * lax.rsqrt(jnp.mean(widened * widened, axis=1, keepdims=True) + epsilon)
    ).astype(jnp.bfloat16)
    count, features = q_ref.shape
    language = r_ref[...]
    onehot = (lax.broadcasted_iota(jnp.int32, (langs, count), 0) == language).astype(jnp.float32)
    upto = (
        lax.broadcasted_iota(jnp.int32, (count, count), 0)
        <= lax.broadcasted_iota(jnp.int32, (count, count), 1)
    ).astype(jnp.bfloat16)
    ranks = jnp.dot(onehot.astype(jnp.bfloat16), upto, preferred_element_type=jnp.float32)
    slot = jnp.sum(ranks * onehot, axis=0, keepdims=True).astype(jnp.int32) - 1
    first = slot < MAIN
    main_row = jnp.where(first, language * MAIN + slot, -1)
    out_main[...] = (
        jnp.dot(
            place((langs * MAIN, count), main_row).astype(jnp.bfloat16), unit,
            preferred_element_type=jnp.float32,
        ).astype(jnp.bfloat16).reshape(out_main.shape)
    )
    packed = jnp.zeros((langs * PACK, LANES), jnp.float32)
    for c in range(features // LANES):
        rest_row = jnp.where(first, -1, language * PACK + c * REST + slot - MAIN)
        packed += jnp.dot(
            place((langs * PACK, count), rest_row).astype(jnp.bfloat16),
            unit[:, c * LANES:(c + 1) * LANES], preferred_element_type=jnp.float32,
        )
    out_rest[...] = packed.astype(jnp.bfloat16).reshape(out_rest.shape)
    pl.semaphore_wait(barrier, langs - 1 + shard_count - 1)

    def over_lang(source, target, send_sems, recv_sems, d, k):
        to = later(d, k)
        return pltpu.make_async_remote_copy(
            src_ref=source.at[to], dst_ref=target.at[my_lang],
            send_sem=send_sems.at[to], recv_sem=recv_sems.at[my_lang],
            device_id=(to, my_shard), device_id_type=MESH,
        )

    def from_lang(source, target, send_sems, recv_sems, d, k):
        origin = earlier(d, k)
        return pltpu.make_async_remote_copy(
            src_ref=source.at[origin], dst_ref=target.at[origin],
            send_sem=send_sems.at[origin], recv_sem=recv_sems.at[origin],
            device_id=(origin, my_shard), device_id_type=MESH,
        )

    a_main = (out_main, all_main.at[my_shard], am_send, am_recv)
    a_rest = (out_rest, all_rest.at[my_shard], ar_send, ar_recv)
    z_main = (ret_main, back_main, zm_send, zm_recv)
    z_rest = (ret_rest, back_rest, zr_send, zr_recv)
    b_main = (all_main, bm_send, bm_recv)
    b_rest = (all_rest, br_send, br_recv)

    def over_shard(source, every, send_sems, recv_sems, lang, step):
        to = next_shard(step)
        return pltpu.make_async_remote_copy(
            src_ref=source, dst_ref=every.at[my_shard, lang],
            send_sem=send_sems.at[to, lang], recv_sem=recv_sems.at[my_shard, lang],
            device_id=(my_lang, to), device_id_type=MESH,
        )

    def from_shard(every, send_sems, recv_sems, lang, step):
        origin = last_shard(step)
        return pltpu.make_async_remote_copy(
            src_ref=every.at[origin, lang], dst_ref=every.at[origin, lang],
            send_sem=send_sems.at[origin, lang], recv_sem=recv_sems.at[origin, lang],
            device_id=(my_lang, origin), device_id_type=MESH,
        )

    for step in range(1, shard_count):
        over_shard(out_main.at[my_lang], *b_main, my_lang, step).start()
    for d, k in steps:
        over_lang(*a_main, d, k).start()
        over_lang(*a_rest, d, k).start()
    for step in range(1, shard_count):
        over_shard(out_rest.at[my_lang], *b_rest, my_lang, step).start()
    all_main[my_shard, my_lang] = out_main[my_lang]
    all_rest[my_shard, my_lang] = out_rest[my_lang]

    def forward(d, k):
        lang = earlier(d, k)
        from_lang(*a_main, d, k).wait_recv()
        for step in range(1, shard_count):
            over_shard(all_main.at[my_shard, lang], *b_main, lang, step).start()
        from_lang(*a_rest, d, k).wait_recv()
        for step in range(1, shard_count):
            over_shard(all_rest.at[my_shard, lang], *b_rest, lang, step).start()

    def forward_group(d):
        for k in range(group):
            forward(d, k)

    for k in range(1, group):
        forward(0, k)

    un_main[...] = place((langs * MAIN, count), main_row).T
    un_rest[...] = place(
        (langs * TAIL, count), jnp.where(first, -1, language * TAIL + slot - MAIN)
    ).T
    ret_rest[...] = jnp.zeros_like(ret_rest)

    ahead = min(2, groups - 1)
    for d in range(1, ahead + 1):
        forward_group(d)
    load.wait()
    sign = (1 - 2 * lax.rem(my_shard, 2)).astype(jnp.float32)

    def answer(c, step):
        to = next_shard(step)
        return pltpu.make_async_remote_copy(
            src_ref=result.at[c, to], dst_ref=cand.at[my_shard, c],
            send_sem=r_send.at[to, c], recv_sem=r_recv.at[my_shard, c],
            device_id=(my_lang, to), device_id_type=MESH,
        )

    def answered(c, step):
        origin = last_shard(step)
        return pltpu.make_async_remote_copy(
            src_ref=result.at[c, origin], dst_ref=cand.at[origin, c],
            send_sem=r_send.at[origin, c], recv_sem=r_recv.at[origin, c],
            device_id=(my_lang, origin), device_id_type=MESH,
        )

    def put(i, v):
        t[pl.ds(i, 1), :] = v[i % SUB:i % SUB + 1, :]

    def score(c, carry):
        @pl.when(c < groups)
        def _():
            base = lax.rem(my_group + groups - c, groups) * group
            for k in range(group):
                for step in range(1, shard_count):
                    from_shard(*b_main, base + k, step).wait_recv()
            for s in range(shard_count):
                block[s * part:(s + 1) * part, :] = all_main[s, pl.ds(base, group)].reshape(
                    part, features
                )

        @pl.when(c == groups)
        def _():
            for lang in range(langs):
                for step in range(1, shard_count):
                    from_shard(*b_rest, lang, step).wait_recv()

        @pl.when(c >= groups)
        def _():
            begin = (c - groups) * tail_langs
            shape = (LANES, shard_count * tail_langs * PACK)
            row = lax.broadcasted_iota(jnp.int32, shape, 0)
            column = lax.broadcasted_iota(jnp.int32, shape, 1)
            pieces = all_rest[:, pl.ds(begin, tail_langs)].reshape(shape[1], LANES)
            for f in range(features // LANES):
                pick = (column == row // REST * PACK + f * REST + row % REST).astype(jnp.bfloat16)
                block[:, f * LANES:(f + 1) * LANES] = jnp.dot(
                    pick, pieces, preferred_element_type=jnp.float32
                ).astype(jnp.bfloat16)

        scores = lax.dot_general(
            corpus[...], block[...], (((1,), (1,)), ((), ())), preferred_element_type=jnp.float32
        )
        x[...] = scores.reshape(x.shape)
        top_block(x, y, put, sign)
        result[c] = (t[...] * sign).T.reshape(shard_count, part, TOPK)
        for step in range(1, shard_count):
            answer(c, step).start()
        cand[my_shard, c] = result[c, my_shard]

        @pl.when(c + ahead + 1 < groups)
        def _():
            forward_group(c + ahead + 1)

        return carry

    lax.fori_loop(0, chunks, score, 0)

    def settle(c, carry):
        for step in range(1, shard_count):
            answered(c, step).wait_recv()
        return carry

    def merge(begin, end):
        lists = [
            cand[s, begin:end].reshape((end - begin) * part, TOPK) for s in range(shard_count)
        ]
        while len(lists) > 1:
            lists = [
                merge_lanes(jnp.maximum(lists[2 * j], lists[2 * j + 1]), j % 2 == 0)
                for j in range(len(lists) // 2)
            ]
        return lists[0]

    lax.fori_loop(0, groups, settle, 0)
    merged = merge(0, groups)
    for d in range(groups):
        base = lax.rem(my_group + groups - d, groups) * group
        ret_main[pl.ds(base, group)] = merged[d * part:(d + 1) * part].reshape(group, MAIN, TOPK)
    for d, k in steps:
        over_lang(*z_main, d, k).start()
    lax.fori_loop(groups, chunks, settle, 0)
    merged = merge(groups, chunks)
    for lang in range(langs):
        ret_rest[lang, 0:REST, :] = merged[lang * REST:(lang + 1) * REST, :]
    for d, k in steps:
        over_lang(*z_rest, d, k).start()
    back_main[my_lang] = ret_main[my_lang]
    back_rest[my_lang] = ret_rest[my_lang]

    def drain(lang, carry):
        for step in range(1, shard_count):
            over_shard(all_main.at[my_shard, lang], *b_main, lang, step).wait_send()
            over_shard(all_rest.at[my_shard, lang], *b_rest, lang, step).wait_send()
        return carry

    def drain_answers(c, carry):
        for step in range(1, shard_count):
            answer(c, step).wait_send()
        return carry

    lax.fori_loop(0, langs, drain, 0)
    lax.fori_loop(0, chunks, drain_answers, 0)
    for d, k in steps:
        over_lang(*a_main, d, k).wait_send()
        over_lang(*a_rest, d, k).wait_send()
    for d, k in steps:
        from_lang(*z_main, d, k).wait_recv()
    upper = jnp.dot(
        un_main[...], back_main[...].reshape(langs * MAIN, TOPK),
        preferred_element_type=jnp.float32, precision=lax.Precision.HIGHEST,
    )
    for d, k in steps:
        from_lang(*z_rest, d, k).wait_recv()
    o_ref[...] = upper + jnp.dot(
        un_rest[...], back_rest[...].reshape(langs * TAIL, TOPK),
        preferred_element_type=jnp.float32, precision=lax.Precision.HIGHEST,
    )
    for d, k in steps:
        over_lang(*z_main, d, k).wait_send()
        over_lang(*z_rest, d, k).wait_send()


def shards(queries, routes, corpus):
    langs = lax.axis_size("lang")
    shard_count = lax.axis_size("shard")
    count, features = queries.shape
    part = LANES // shard_count
    chunks = langs * CAP // part
    dma = pltpu.SemaphoreType.DMA
    f32, bf16 = jnp.float32, jnp.bfloat16
    return pl.pallas_call(
        functools.partial(kernel, langs, shard_count),
        out_shape=jax.ShapeDtypeStruct((count, TOPK), f32),
        in_specs=[
            pl.BlockSpec(memory_space=pltpu.VMEM),
            pl.BlockSpec(memory_space=pltpu.VMEM),
            pl.BlockSpec(memory_space=pl.ANY),
        ],
        out_specs=pl.BlockSpec(memory_space=pltpu.VMEM),
        scratch_shapes=[
            pltpu.VMEM(corpus.shape, bf16),
            pltpu.VMEM((langs, MAIN, features), bf16),
            pltpu.VMEM((langs, PACK, LANES), bf16),
            pltpu.VMEM((shard_count, langs, MAIN, features), bf16),
            pltpu.VMEM((shard_count, langs, PACK, LANES), bf16),
            pltpu.VMEM((LANES, features), bf16),
            pltpu.VMEM((TOPK, SUB, LANES), f32),
            pltpu.VMEM((TOPK, SUB, LANES), f32),
            pltpu.VMEM((TOPK, LANES), f32),
            pltpu.VMEM((chunks, shard_count, part, TOPK), f32),
            pltpu.VMEM((shard_count, chunks, part, TOPK), f32),
            pltpu.VMEM((langs, MAIN, TOPK), f32),
            pltpu.VMEM((langs, TAIL, TOPK), f32),
            pltpu.VMEM((langs, MAIN, TOPK), f32),
            pltpu.VMEM((langs, TAIL, TOPK), f32),
            pltpu.VMEM((count, langs * MAIN), f32),
            pltpu.VMEM((count, langs * TAIL), f32),
            dma, *[dma((langs,))] * 4, *[dma((shard_count, langs))] * 4,
            *[dma((shard_count, chunks))] * 2, *[dma((langs,))] * 4,
        ],
        compiler_params=pltpu.CompilerParams(collective_id=0, has_side_effects=True),
    )(queries, routes.reshape(1, count), corpus)


def solution(mesh):
    placed = (P(("lang", "shard"), None), P(("lang", "shard"), None), P(("lang", "shard"), None))
    return jax.shard_map(
        shards, mesh=mesh, in_specs=placed, out_specs=P(("lang", "shard"), None), check_vma=False
    )
```

```python
import functools
import jax
import jax.numpy as jnp
from jax import lax
from jax.experimental import pallas as pl
from jax.experimental.pallas import tpu as pltpu
from jax.sharding import PartitionSpec as P

CAP = 20
TOPK = 128
LANES = 128
SUB = 8
PART = 32
MAIN = 16
REST = CAP - MAIN
PACK = 32
TAIL = 8
MESH = pl.DeviceIdType.MESH


epsilon = 1e-06


def exchange(values, i, j):
    values[i], values[j] = jnp.maximum(values[i], values[j]), jnp.minimum(values[i], values[j])


def sort_down(values):
    values = list(values)
    n = len(values)
    p = 1
    while p < n:
        k = p
        while k >= 1:
            for j in range(k % p, n - k, 2 * k):
                for i in range(min(k, n - j - k)):
                    if (i + j) // (2 * p) == (i + j + k) // (2 * p):
                        exchange(values, i + j, i + j + k)
            k //= 2
        p *= 2
    return values


def bitonic_down(values):
    values = list(values)
    d = len(values) // 2
    while d:
        for i in range(len(values)):
            if not i & d:
                exchange(values, i, i + d)
        d //= 2
    return values


def top_block(x, y, put, sign):
    n = TOPK
    for g in range(n // PART):
        run = sort_down([x[g * PART + i] for i in range(PART)])
        for i in range(PART):
            x[g * PART + (i if g % 2 == 0 else PART - 1 - i)] = run[i]
    for g in range(2):
        base = g * 2 * PART
        for half, take in enumerate((jnp.maximum, jnp.minimum)):
            run = bitonic_down([take(x[base + i], x[base + PART + i]) for i in range(PART)])
            for i in range(PART):
                at = half * PART + i
                y[base + (at if g == 0 else 2 * PART - 1 - at)] = run[i]

    def quarters(source, target, pick):
        for i in range(PART):
            four = [pick(source, i + PART * j) for j in range(4)]
            four = bitonic_down(four)
            for j in range(4):
                target[i + PART * j] = four[j]

    def finish(source, store):
        for g in range(4):
            run = bitonic_down([source[g * PART + i] for i in range(PART)])
            for i in range(PART):
                store(g * PART + i, run[i])

    def keep(target):
        def store(i, v):
            target[i] = v
        return store

    quarters(y, x, lambda s, i: s[i])
    finish(x, keep(y))
    source, target = y, x
    for shift in (4, 2, 1):
        def pick(s, i, shift=shift):
            best = jnp.maximum(s[i], pltpu.roll(s[n - 1 - i], shift, 0))
            return best * sign if shift == 1 else best

        quarters(source, target, pick)
        finish(target, put if shift == 1 else keep(source))


def merge_lanes(values, down):
    lane = lax.broadcasted_iota(jnp.int32, values.shape, 1)
    d = LANES // 2
    while d:
        above = pltpu.roll(values, LANES - d, 1)
        below = pltpu.roll(values, d, 1)
        low = (lane & d) == 0
        if down:
            values = jnp.where(low, jnp.maximum(values, above), jnp.minimum(values, below))
        else:
            values = jnp.where(low, jnp.minimum(values, above), jnp.maximum(values, below))
        d //= 2
    return values


def place(shape, slots):
    return (lax.broadcasted_iota(jnp.int32, shape, 0) == slots).astype(jnp.float32)


def kernel(
    langs, shard_count, q_ref, r_ref, c_hbm, o_ref,
    corpus, out_main, out_rest, all_main, all_rest, block, x, y, t, result, cand,
    ret_main, ret_rest, back_main, back_rest, un_main, un_rest,
    c_sem, am_send, am_recv, ar_send, ar_recv, bm_send, bm_recv, br_send, br_recv,
    r_send, r_recv, zm_send, zm_recv, zr_send, zr_recv,
):
    my_lang = lax.axis_index("lang")
    my_shard = lax.axis_index("shard")
    group = LANES // MAIN // shard_count
    groups = langs // group
    tails = langs * REST * shard_count // LANES
    tail_langs = langs // tails
    part = LANES // shard_count
    chunks = groups + tails
    my_group, my_place = my_lang // group, lax.rem(my_lang, group)
    steps = [(d, k) for d in range(groups) for k in range(group) if d or k]

    load = pltpu.make_async_copy(c_hbm, corpus, c_sem)
    load.start()

    def later(d, k):
        return lax.rem(my_group + d, groups) * group + lax.rem(my_place + k, group)

    def earlier(d, k):
        return lax.rem(my_group + groups - d, groups) * group + lax.rem(my_place + group - k, group)

    square = shard_count == 4
    hops = (1, 2) if square else range(1, shard_count)

    def across(step):
        return my_shard + step - 2 * step * lax.rem(my_shard // step, 2)

    def next_shard(step):
        return lax.rem(my_shard + step, shard_count)

    def last_shard(step):
        return lax.rem(my_shard + shard_count - step, shard_count)

    barrier = pltpu.get_barrier_semaphore()
    for d, k in steps:
        pl.semaphore_signal(barrier, inc=1, device_id=(later(d, k), my_shard), device_id_type=MESH)
    for step in range(1, shard_count):
        pl.semaphore_signal(
            barrier, inc=1, device_id=(my_lang, next_shard(step)), device_id_type=MESH
        )

    widened = q_ref[...].astype(jnp.float32)
    unit = (
        widened * lax.rsqrt(jnp.mean(widened * widened, axis=1, keepdims=True) + epsilon)
    ).astype(jnp.bfloat16)
    count, features = q_ref.shape
    language = r_ref[...]
    onehot = (lax.broadcasted_iota(jnp.int32, (langs, count), 0) == language).astype(jnp.float32)
    upto = (
        lax.broadcasted_iota(jnp.int32, (count, count), 0)
        <= lax.broadcasted_iota(jnp.int32, (count, count), 1)
    ).astype(jnp.bfloat16)
    ranks = jnp.dot(onehot.astype(jnp.bfloat16), upto, preferred_element_type=jnp.float32)
    slot = jnp.sum(ranks * onehot, axis=0, keepdims=True).astype(jnp.int32) - 1
    first = slot < MAIN
    main_row = jnp.where(first, language * MAIN + slot, -1)
    out_main[...] = (
        jnp.dot(
            place((langs * MAIN, count), main_row).astype(jnp.bfloat16), unit,
            preferred_element_type=jnp.float32,
        ).astype(jnp.bfloat16).reshape(out_main.shape)
    )
    pl.semaphore_wait(barrier, langs - 1 + shard_count - 1)

    def over_lang(source, target, send_sems, recv_sems, d, k):
        to = later(d, k)
        return pltpu.make_async_remote_copy(
            src_ref=source.at[to], dst_ref=target.at[my_lang],
            send_sem=send_sems.at[to], recv_sem=recv_sems.at[my_lang],
            device_id=(to, my_shard), device_id_type=MESH,
        )

    def from_lang(source, target, send_sems, recv_sems, d, k):
        origin = earlier(d, k)
        return pltpu.make_async_remote_copy(
            src_ref=source.at[origin], dst_ref=target.at[origin],
            send_sem=send_sems.at[origin], recv_sem=recv_sems.at[origin],
            device_id=(origin, my_shard), device_id_type=MESH,
        )

    a_main = (out_main, all_main.at[my_shard], am_send, am_recv)
    a_rest = (out_rest, all_rest.at[my_shard], ar_send, ar_recv)
    z_main = (ret_main, back_main, zm_send, zm_recv)
    z_rest = (ret_rest, back_rest, zr_send, zr_recv)
    b_main = (all_main, bm_send, bm_recv)
    b_rest = (all_rest, br_send, br_recv)

    def over_shard(source, every, send_sems, recv_sems, lang, step):
        to = across(step) if square else next_shard(step)
        return pltpu.make_async_remote_copy(
            src_ref=source, dst_ref=every.at[my_shard, lang],
            send_sem=send_sems.at[to, lang], recv_sem=recv_sems.at[my_shard, lang],
            device_id=(my_lang, to), device_id_type=MESH,
        )

    def relay(every, send_sems, recv_sems, lang):
        turn = 1 + lax.rem(lang, 2)
        origin, to = across(turn), across(3 - turn)
        return pltpu.make_async_remote_copy(
            src_ref=every.at[origin, lang], dst_ref=every.at[origin, lang],
            send_sem=send_sems.at[my_shard, lang], recv_sem=recv_sems.at[origin, lang],
            device_id=(my_lang, to), device_id_type=MESH,
        )

    def relay_group(d):
        for k in range(group):
            lang = earlier(d, k)
            for b in (b_main, b_rest):
                from_origin(*b, lang, across(1 + lax.rem(lang, 2))).wait_recv()
                relay(*b, lang).start()

    def await_others(b, lang):
        if square:
            from_origin(*b, lang, across(2 - lax.rem(lang, 2))).wait_recv()
            from_origin(*b, lang, 3 - my_shard).wait_recv()
        else:
            for step in range(1, shard_count):
                from_origin(*b, lang, last_shard(step)).wait_recv()

    def from_origin(every, send_sems, recv_sems, lang, origin):
        return pltpu.make_async_remote_copy(
            src_ref=every.at[origin, lang], dst_ref=every.at[origin, lang],
            send_sem=send_sems.at[origin, lang], recv_sem=recv_sems.at[origin, lang],
            device_id=(my_lang, origin), device_id_type=MESH,
        )

    for step in hops:
        over_shard(out_main.at[my_lang], *b_main, my_lang, step).start()
    for d, k in steps:
        over_lang(*a_main, d, k).start()
    packed = jnp.zeros((langs * PACK, LANES), jnp.float32)
    for c in range(features // LANES):
        rest_row = jnp.where(first, -1, language * PACK + c * REST + slot - MAIN)
        packed += jnp.dot(
            place((langs * PACK, count), rest_row).astype(jnp.bfloat16),
            unit[:, c * LANES:(c + 1) * LANES], preferred_element_type=jnp.float32,
        )
    out_rest[...] = packed.astype(jnp.bfloat16).reshape(out_rest.shape)
    for d, k in steps:
        over_lang(*a_rest, d, k).start()
    for step in hops:
        over_shard(out_rest.at[my_lang], *b_rest, my_lang, step).start()
    all_main[my_shard, my_lang] = out_main[my_lang]
    all_rest[my_shard, my_lang] = out_rest[my_lang]

    def forward(d, k):
        lang = earlier(d, k)
        from_lang(*a_main, d, k).wait_recv()
        for step in hops:
            over_shard(all_main.at[my_shard, lang], *b_main, lang, step).start()
        from_lang(*a_rest, d, k).wait_recv()
        for step in hops:
            over_shard(all_rest.at[my_shard, lang], *b_rest, lang, step).start()

    def forward_group(d):
        for k in range(group):
            forward(d, k)

    for k in range(1, group):
        forward(0, k)

    un_main[...] = place((langs * MAIN, count), main_row).T
    un_rest[...] = place(
        (langs * TAIL, count), jnp.where(first, -1, language * TAIL + slot - MAIN)
    ).T
    ret_rest[...] = jnp.zeros_like(ret_rest)

    ahead = min(3 if square else 2, groups - 1)
    for d in range(1, ahead + 1):
        forward_group(d)
        if square and d <= 2:
            relay_group(d - 1)
    load.wait()
    sign = (1 - 2 * lax.rem(my_shard, 2)).astype(jnp.float32)

    def answer(c, step):
        to = next_shard(step)
        return pltpu.make_async_remote_copy(
            src_ref=result.at[c, to], dst_ref=cand.at[my_shard, c],
            send_sem=r_send.at[to, c], recv_sem=r_recv.at[my_shard, c],
            device_id=(my_lang, to), device_id_type=MESH,
        )

    def answered(c, step):
        origin = last_shard(step)
        return pltpu.make_async_remote_copy(
            src_ref=result.at[c, origin], dst_ref=cand.at[origin, c],
            send_sem=r_send.at[origin, c], recv_sem=r_recv.at[origin, c],
            device_id=(my_lang, origin), device_id_type=MESH,
        )

    def put(i, v):
        t[pl.ds(i, 1), :] = v[i % SUB:i % SUB + 1, :]

    def score(c, carry):
        if square:
            @pl.when(c + 2 < groups)
            def _():
                relay_group(c + 2)

        @pl.when(c < groups)
        def _():
            base = lax.rem(my_group + groups - c, groups) * group
            for k in range(group):
                await_others(b_main, base + k)
            for s in range(shard_count):
                block[s * part:(s + 1) * part, :] = all_main[s, pl.ds(base, group)].reshape(
                    part, features
                )

        @pl.when(c == groups)
        def _():
            for lang in range(langs):
                await_others(b_rest, lang)

        @pl.when(c >= groups)
        def _():
            begin = (c - groups) * tail_langs
            shape = (LANES, shard_count * tail_langs * PACK)
            row = lax.broadcasted_iota(jnp.int32, shape, 0)
            column = lax.broadcasted_iota(jnp.int32, shape, 1)
            pieces = all_rest[:, pl.ds(begin, tail_langs)].reshape(shape[1], LANES)
            for f in range(features // LANES):
                pick = (column == row // REST * PACK + f * REST + row % REST).astype(jnp.bfloat16)
                block[:, f * LANES:(f + 1) * LANES] = jnp.dot(
                    pick, pieces, preferred_element_type=jnp.float32
                ).astype(jnp.bfloat16)

        scores = lax.dot_general(
            corpus[...], block[...], (((1,), (1,)), ((), ())), preferred_element_type=jnp.float32
        )
        x[...] = scores.reshape(x.shape)
        top_block(x, y, put, sign)
        result[c] = (t[...] * sign).T.reshape(shard_count, part, TOPK)
        for step in range(1, shard_count):
            answer(c, step).start()
        cand[my_shard, c] = result[c, my_shard]

        @pl.when(c + ahead + 1 < groups)
        def _():
            forward_group(c + ahead + 1)

        return carry

    lax.fori_loop(0, chunks, score, 0)

    def settle(c, carry):
        for step in range(1, shard_count):
            answered(c, step).wait_recv()
        return carry

    def merge(begin, end):
        lists = [
            cand[s, begin:end].reshape((end - begin) * part, TOPK) for s in range(shard_count)
        ]
        while len(lists) > 1:
            lists = [
                merge_lanes(jnp.maximum(lists[2 * j], lists[2 * j + 1]), j % 2 == 0)
                for j in range(len(lists) // 2)
            ]
        return lists[0]

    lax.fori_loop(0, groups, settle, 0)
    merged = merge(0, groups)
    for d in range(groups):
        base = lax.rem(my_group + groups - d, groups) * group
        ret_main[pl.ds(base, group)] = merged[d * part:(d + 1) * part].reshape(group, MAIN, TOPK)
    for d, k in steps:
        over_lang(*z_main, d, k).start()
    lax.fori_loop(groups, chunks, settle, 0)
    merged = merge(groups, chunks)
    for lang in range(langs):
        ret_rest[lang, 0:REST, :] = merged[lang * REST:(lang + 1) * REST, :]
    for d, k in steps:
        over_lang(*z_rest, d, k).start()
    back_main[my_lang] = ret_main[my_lang]
    back_rest[my_lang] = ret_rest[my_lang]

    def drain(lang, carry):
        for step in hops:
            over_shard(all_main.at[my_shard, lang], *b_main, lang, step).wait_send()
            over_shard(all_rest.at[my_shard, lang], *b_rest, lang, step).wait_send()
        if square:
            relay(*b_main, lang).wait_send()
            relay(*b_rest, lang).wait_send()
        return carry

    def drain_answers(c, carry):
        for step in range(1, shard_count):
            answer(c, step).wait_send()
        return carry

    lax.fori_loop(0, langs, drain, 0)
    lax.fori_loop(0, chunks, drain_answers, 0)
    for d, k in steps:
        over_lang(*a_main, d, k).wait_send()
        over_lang(*a_rest, d, k).wait_send()
    for d, k in steps:
        from_lang(*z_main, d, k).wait_recv()
    upper = jnp.dot(
        un_main[...], back_main[...].reshape(langs * MAIN, TOPK),
        preferred_element_type=jnp.float32, precision=lax.Precision.HIGHEST,
    )
    for d, k in steps:
        from_lang(*z_rest, d, k).wait_recv()
    o_ref[...] = upper + jnp.dot(
        un_rest[...], back_rest[...].reshape(langs * TAIL, TOPK),
        preferred_element_type=jnp.float32, precision=lax.Precision.HIGHEST,
    )
    for d, k in steps:
        over_lang(*z_main, d, k).wait_send()
        over_lang(*z_rest, d, k).wait_send()


def shards(queries, routes, corpus):
    langs = lax.axis_size("lang")
    shard_count = lax.axis_size("shard")
    count, features = queries.shape
    part = LANES // shard_count
    chunks = langs * CAP // part
    dma = pltpu.SemaphoreType.DMA
    f32, bf16 = jnp.float32, jnp.bfloat16
    return pl.pallas_call(
        functools.partial(kernel, langs, shard_count),
        out_shape=jax.ShapeDtypeStruct((count, TOPK), f32),
        in_specs=[
            pl.BlockSpec(memory_space=pltpu.VMEM),
            pl.BlockSpec(memory_space=pltpu.VMEM),
            pl.BlockSpec(memory_space=pl.ANY),
        ],
        out_specs=pl.BlockSpec(memory_space=pltpu.VMEM),
        scratch_shapes=[
            pltpu.VMEM(corpus.shape, bf16),
            pltpu.VMEM((langs, MAIN, features), bf16),
            pltpu.VMEM((langs, PACK, LANES), bf16),
            pltpu.VMEM((shard_count, langs, MAIN, features), bf16),
            pltpu.VMEM((shard_count, langs, PACK, LANES), bf16),
            pltpu.VMEM((LANES, features), bf16),
            pltpu.VMEM((TOPK, SUB, LANES), f32),
            pltpu.VMEM((TOPK, SUB, LANES), f32),
            pltpu.VMEM((TOPK, LANES), f32),
            pltpu.VMEM((chunks, shard_count, part, TOPK), f32),
            pltpu.VMEM((shard_count, chunks, part, TOPK), f32),
            pltpu.VMEM((langs, MAIN, TOPK), f32),
            pltpu.VMEM((langs, TAIL, TOPK), f32),
            pltpu.VMEM((langs, MAIN, TOPK), f32),
            pltpu.VMEM((langs, TAIL, TOPK), f32),
            pltpu.VMEM((count, langs * MAIN), f32),
            pltpu.VMEM((count, langs * TAIL), f32),
            dma, *[dma((langs,))] * 4, *[dma((shard_count, langs))] * 4,
            *[dma((shard_count, chunks))] * 2, *[dma((langs,))] * 4,
        ],
        compiler_params=pltpu.CompilerParams(collective_id=0, has_side_effects=True),
    )(queries, routes.reshape(1, count), corpus)


def solution(mesh):
    placed = (P(("lang", "shard"), None), P(("lang", "shard"), None), P(("lang", "shard"), None))
    return jax.shard_map(
        shards, mesh=mesh, in_specs=placed, out_specs=P(("lang", "shard"), None), check_vma=False
    )
```

```python
import functools
import jax
import jax.numpy as jnp
from jax import lax
from jax.experimental import pallas as pl
from jax.experimental.pallas import tpu as pltpu
from jax.sharding import PartitionSpec as P

CAP = 20
TOPK = 128
LANES = 128
SUB = 8
PART = 32
MAIN = 16
REST = CAP - MAIN
PACK = 32
TAIL = 8
MESH = pl.DeviceIdType.MESH


epsilon = 1e-06


def exchange(values, i, j):
    values[i], values[j] = jnp.maximum(values[i], values[j]), jnp.minimum(values[i], values[j])


def sort_down(values):
    values = list(values)
    n = len(values)
    p = 1
    while p < n:
        k = p
        while k >= 1:
            for j in range(k % p, n - k, 2 * k):
                for i in range(min(k, n - j - k)):
                    if (i + j) // (2 * p) == (i + j + k) // (2 * p):
                        exchange(values, i + j, i + j + k)
            k //= 2
        p *= 2
    return values


def bitonic_down(values):
    values = list(values)
    d = len(values) // 2
    while d:
        for i in range(len(values)):
            if not i & d:
                exchange(values, i, i + d)
        d //= 2
    return values


def top_block(x, y, put, sign):
    n = TOPK
    for g in range(n // PART):
        run = sort_down([x[g * PART + i] for i in range(PART)])
        for i in range(PART):
            x[g * PART + (i if g % 2 == 0 else PART - 1 - i)] = run[i]
    for g in range(2):
        base = g * 2 * PART
        for half, take in enumerate((jnp.maximum, jnp.minimum)):
            run = bitonic_down([take(x[base + i], x[base + PART + i]) for i in range(PART)])
            for i in range(PART):
                at = half * PART + i
                y[base + (at if g == 0 else 2 * PART - 1 - at)] = run[i]

    def quarters(source, target, pick):
        for i in range(PART):
            four = [pick(source, i + PART * j) for j in range(4)]
            four = bitonic_down(four)
            for j in range(4):
                target[i + PART * j] = four[j]

    def finish(source, store):
        for g in range(4):
            run = bitonic_down([source[g * PART + i] for i in range(PART)])
            for i in range(PART):
                store(g * PART + i, run[i])

    def keep(target):
        def store(i, v):
            target[i] = v
        return store

    quarters(y, x, lambda s, i: s[i])
    finish(x, keep(y))
    source, target = y, x
    for shift in (4, 2, 1):
        def pick(s, i, shift=shift):
            best = jnp.maximum(s[i], pltpu.roll(s[n - 1 - i], shift, 0))
            return best * sign if shift == 1 else best

        quarters(source, target, pick)
        finish(target, put if shift == 1 else keep(source))


def merge_lanes(values, down):
    lane = lax.broadcasted_iota(jnp.int32, values.shape, 1)
    d = LANES // 2
    while d:
        above = pltpu.roll(values, LANES - d, 1)
        below = pltpu.roll(values, d, 1)
        low = (lane & d) == 0
        if down:
            values = jnp.where(low, jnp.maximum(values, above), jnp.minimum(values, below))
        else:
            values = jnp.where(low, jnp.minimum(values, above), jnp.maximum(values, below))
        d //= 2
    return values


def place(shape, slots):
    return (lax.broadcasted_iota(jnp.int32, shape, 0) == slots).astype(jnp.float32)


def kernel(
    langs, shard_count, q_ref, r_ref, c_hbm, o_ref,
    corpus, out_main, out_rest, all_main, all_rest, block, x, y, t, result, cand,
    ret_main, ret_rest, back_main, back_rest, un_main, un_rest,
    c_sem, am_send, am_recv, ar_send, ar_recv, bm_send, bm_recv, br_send, br_recv,
    r_send, r_recv, zm_send, zm_recv, zr_send, zr_recv,
):
    my_lang = lax.axis_index("lang")
    my_shard = lax.axis_index("shard")
    group = LANES // MAIN // shard_count
    groups = langs // group
    tails = langs * REST * shard_count // LANES
    tail_langs = langs // tails
    part = LANES // shard_count
    chunks = groups + tails
    my_group, my_place = my_lang // group, lax.rem(my_lang, group)
    steps = [(d, k) for d in range(groups) for k in range(group) if d or k]

    load = pltpu.make_async_copy(c_hbm, corpus, c_sem)
    load.start()

    def later(d, k):
        return lax.rem(my_group + d, groups) * group + lax.rem(my_place + k, group)

    def earlier(d, k):
        return lax.rem(my_group + groups - d, groups) * group + lax.rem(my_place + group - k, group)

    def next_shard(step):
        return lax.rem(my_shard + step, shard_count)

    def last_shard(step):
        return lax.rem(my_shard + shard_count - step, shard_count)

    barrier = pltpu.get_barrier_semaphore()
    for d, k in steps:
        pl.semaphore_signal(barrier, inc=1, device_id=(later(d, k), my_shard), device_id_type=MESH)
    for step in range(1, shard_count):
        pl.semaphore_signal(
            barrier, inc=1, device_id=(my_lang, next_shard(step)), device_id_type=MESH
        )

    widened = q_ref[...].astype(jnp.float32)
    unit = (
        widened * lax.rsqrt(jnp.mean(widened * widened, axis=1, keepdims=True) + epsilon)
    ).astype(jnp.bfloat16)
    count, features = q_ref.shape
    language = r_ref[...]
    onehot = (lax.broadcasted_iota(jnp.int32, (langs, count), 0) == language).astype(jnp.float32)
    upto = (
        lax.broadcasted_iota(jnp.int32, (count, count), 0)
        <= lax.broadcasted_iota(jnp.int32, (count, count), 1)
    ).astype(jnp.bfloat16)
    ranks = jnp.dot(onehot.astype(jnp.bfloat16), upto, preferred_element_type=jnp.float32)
    slot = jnp.sum(ranks * onehot, axis=0, keepdims=True).astype(jnp.int32) - 1
    first = slot < MAIN
    main_row = jnp.where(first, language * MAIN + slot, -1)
    out_main[...] = (
        jnp.dot(
            place((langs * MAIN, count), main_row).astype(jnp.bfloat16), unit,
            preferred_element_type=jnp.float32,
        ).astype(jnp.bfloat16).reshape(out_main.shape)
    )
    packed = jnp.zeros((langs * PACK, LANES), jnp.float32)
    for c in range(features // LANES):
        rest_row = jnp.where(first, -1, language * PACK + c * REST + slot - MAIN)
        packed += jnp.dot(
            place((langs * PACK, count), rest_row).astype(jnp.bfloat16),
            unit[:, c * LANES:(c + 1) * LANES], preferred_element_type=jnp.float32,
        )
    out_rest[...] = packed.astype(jnp.bfloat16).reshape(out_rest.shape)
    pl.semaphore_wait(barrier, langs - 1 + shard_count - 1)

    def over_lang(source, target, send_sems, recv_sems, d, k):
        to = later(d, k)
        return pltpu.make_async_remote_copy(
            src_ref=source.at[to], dst_ref=target.at[my_lang],
            send_sem=send_sems.at[to], recv_sem=recv_sems.at[my_lang],
            device_id=(to, my_shard), device_id_type=MESH,
        )

    def from_lang(source, target, send_sems, recv_sems, d, k):
        origin = earlier(d, k)
        return pltpu.make_async_remote_copy(
            src_ref=source.at[origin], dst_ref=target.at[origin],
            send_sem=send_sems.at[origin], recv_sem=recv_sems.at[origin],
            device_id=(origin, my_shard), device_id_type=MESH,
        )

    a_main = (out_main, all_main.at[my_shard], am_send, am_recv)
    a_rest = (out_rest, all_rest.at[my_shard], ar_send, ar_recv)
    z_main = (ret_main, back_main, zm_send, zm_recv)
    z_rest = (ret_rest, back_rest, zr_send, zr_recv)
    b_main = (all_main, bm_send, bm_recv)
    b_rest = (all_rest, br_send, br_recv)

    def over_shard(source, every, send_sems, recv_sems, lang, step):
        to = next_shard(step)
        return pltpu.make_async_remote_copy(
            src_ref=source, dst_ref=every.at[my_shard, lang],
            send_sem=send_sems.at[to, lang], recv_sem=recv_sems.at[my_shard, lang],
            device_id=(my_lang, to), device_id_type=MESH,
        )

    def from_shard(every, send_sems, recv_sems, lang, step):
        origin = last_shard(step)
        return pltpu.make_async_remote_copy(
            src_ref=every.at[origin, lang], dst_ref=every.at[origin, lang],
            send_sem=send_sems.at[origin, lang], recv_sem=recv_sems.at[origin, lang],
            device_id=(my_lang, origin), device_id_type=MESH,
        )

    for step in range(1, shard_count):
        over_shard(out_main.at[my_lang], *b_main, my_lang, step).start()
    for d, k in steps:
        over_lang(*a_main, d, k).start()
        over_lang(*a_rest, d, k).start()
    for step in range(1, shard_count):
        over_shard(out_rest.at[my_lang], *b_rest, my_lang, step).start()
    all_main[my_shard, my_lang] = out_main[my_lang]
    all_rest[my_shard, my_lang] = out_rest[my_lang]

    def forward(d, k):
        lang = earlier(d, k)
        from_lang(*a_main, d, k).wait_recv()
        for step in range(1, shard_count):
            over_shard(all_main.at[my_shard, lang], *b_main, lang, step).start()
        from_lang(*a_rest, d, k).wait_recv()
        for step in range(1, shard_count):
            over_shard(all_rest.at[my_shard, lang], *b_rest, lang, step).start()

    def forward_group(d):
        for k in range(group):
            forward(d, k)

    for k in range(1, group):
        forward(0, k)

    un_main[...] = place((langs * MAIN, count), main_row).T
    un_rest[...] = place(
        (langs * TAIL, count), jnp.where(first, -1, language * TAIL + slot - MAIN)
    ).T
    ret_rest[...] = jnp.zeros_like(ret_rest)

    ahead = min(3, groups - 1)
    for d in range(1, ahead + 1):
        forward_group(d)
    load.wait()
    sign = (1 - 2 * lax.rem(my_shard, 2)).astype(jnp.float32)

    def answer(c, step):
        to = next_shard(step)
        return pltpu.make_async_remote_copy(
            src_ref=result.at[c, to], dst_ref=cand.at[my_shard, c],
            send_sem=r_send.at[to, c], recv_sem=r_recv.at[my_shard, c],
            device_id=(my_lang, to), device_id_type=MESH,
        )

    def answered(c, step):
        origin = last_shard(step)
        return pltpu.make_async_remote_copy(
            src_ref=result.at[c, origin], dst_ref=cand.at[origin, c],
            send_sem=r_send.at[origin, c], recv_sem=r_recv.at[origin, c],
            device_id=(my_lang, origin), device_id_type=MESH,
        )

    def put(i, v):
        t[pl.ds(i, 1), :] = v[i % SUB:i % SUB + 1, :]

    def score(c, carry):
        @pl.when(c < groups)
        def _():
            base = lax.rem(my_group + groups - c, groups) * group
            for k in range(group):
                for step in range(1, shard_count):
                    from_shard(*b_main, base + k, step).wait_recv()
            for s in range(shard_count):
                block[s * part:(s + 1) * part, :] = all_main[s, pl.ds(base, group)].reshape(
                    part, features
                )

        @pl.when(c == groups)
        def _():
            for lang in range(langs):
                for step in range(1, shard_count):
                    from_shard(*b_rest, lang, step).wait_recv()

        @pl.when(c >= groups)
        def _():
            begin = (c - groups) * tail_langs
            shape = (LANES, shard_count * tail_langs * PACK)
            row = lax.broadcasted_iota(jnp.int32, shape, 0)
            column = lax.broadcasted_iota(jnp.int32, shape, 1)
            pieces = all_rest[:, pl.ds(begin, tail_langs)].reshape(shape[1], LANES)
            for f in range(features // LANES):
                pick = (column == row // REST * PACK + f * REST + row % REST).astype(jnp.bfloat16)
                block[:, f * LANES:(f + 1) * LANES] = jnp.dot(
                    pick, pieces, preferred_element_type=jnp.float32
                ).astype(jnp.bfloat16)

        scores = lax.dot_general(
            corpus[...], block[...], (((1,), (1,)), ((), ())), preferred_element_type=jnp.float32
        )
        x[...] = scores.reshape(x.shape)
        top_block(x, y, put, sign)
        result[c] = (t[...] * sign).T.reshape(shard_count, part, TOPK)
        for step in range(1, shard_count):
            answer(c, step).start()
        cand[my_shard, c] = result[c, my_shard]

        @pl.when(c + ahead + 1 < groups)
        def _():
            forward_group(c + ahead + 1)

        return carry

    lax.fori_loop(0, chunks, score, 0)

    def settle(c, carry):
        for step in range(1, shard_count):
            answered(c, step).wait_recv()
        return carry

    def merge(begin, end):
        lists = [
            cand[s, begin:end].reshape((end - begin) * part, TOPK) for s in range(shard_count)
        ]
        while len(lists) > 1:
            lists = [
                merge_lanes(jnp.maximum(lists[2 * j], lists[2 * j + 1]), j % 2 == 0)
                for j in range(len(lists) // 2)
            ]
        return lists[0]

    lax.fori_loop(0, groups, settle, 0)
    merged = merge(0, groups)
    for d in range(groups):
        base = lax.rem(my_group + groups - d, groups) * group
        ret_main[pl.ds(base, group)] = merged[d * part:(d + 1) * part].reshape(group, MAIN, TOPK)
    for d, k in steps:
        over_lang(*z_main, d, k).start()
    lax.fori_loop(groups, chunks, settle, 0)
    merged = merge(groups, chunks)
    for lang in range(langs):
        ret_rest[lang, 0:REST, :] = merged[lang * REST:(lang + 1) * REST, :]
    for d, k in steps:
        over_lang(*z_rest, d, k).start()
    back_main[my_lang] = ret_main[my_lang]
    back_rest[my_lang] = ret_rest[my_lang]

    def drain(lang, carry):
        for step in range(1, shard_count):
            over_shard(all_main.at[my_shard, lang], *b_main, lang, step).wait_send()
            over_shard(all_rest.at[my_shard, lang], *b_rest, lang, step).wait_send()
        return carry

    def drain_answers(c, carry):
        for step in range(1, shard_count):
            answer(c, step).wait_send()
        return carry

    lax.fori_loop(0, langs, drain, 0)
    lax.fori_loop(0, chunks, drain_answers, 0)
    for d, k in steps:
        over_lang(*a_main, d, k).wait_send()
        over_lang(*a_rest, d, k).wait_send()
    for d, k in steps:
        from_lang(*z_main, d, k).wait_recv()
    upper = jnp.dot(
        un_main[...], back_main[...].reshape(langs * MAIN, TOPK),
        preferred_element_type=jnp.float32, precision=lax.Precision.HIGHEST,
    )
    for d, k in steps:
        from_lang(*z_rest, d, k).wait_recv()
    o_ref[...] = upper + jnp.dot(
        un_rest[...], back_rest[...].reshape(langs * TAIL, TOPK),
        preferred_element_type=jnp.float32, precision=lax.Precision.HIGHEST,
    )
    for d, k in steps:
        over_lang(*z_main, d, k).wait_send()
        over_lang(*z_rest, d, k).wait_send()


def shards(queries, routes, corpus):
    langs = lax.axis_size("lang")
    shard_count = lax.axis_size("shard")
    count, features = queries.shape
    part = LANES // shard_count
    chunks = langs * CAP // part
    dma = pltpu.SemaphoreType.DMA
    f32, bf16 = jnp.float32, jnp.bfloat16
    return pl.pallas_call(
        functools.partial(kernel, langs, shard_count),
        out_shape=jax.ShapeDtypeStruct((count, TOPK), f32),
        in_specs=[
            pl.BlockSpec(memory_space=pltpu.VMEM),
            pl.BlockSpec(memory_space=pltpu.VMEM),
            pl.BlockSpec(memory_space=pl.ANY),
        ],
        out_specs=pl.BlockSpec(memory_space=pltpu.VMEM),
        scratch_shapes=[
            pltpu.VMEM(corpus.shape, bf16),
            pltpu.VMEM((langs, MAIN, features), bf16),
            pltpu.VMEM((langs, PACK, LANES), bf16),
            pltpu.VMEM((shard_count, langs, MAIN, features), bf16),
            pltpu.VMEM((shard_count, langs, PACK, LANES), bf16),
            pltpu.VMEM((LANES, features), bf16),
            pltpu.VMEM((TOPK, SUB, LANES), f32),
            pltpu.VMEM((TOPK, SUB, LANES), f32),
            pltpu.VMEM((TOPK, LANES), f32),
            pltpu.VMEM((chunks, shard_count, part, TOPK), f32),
            pltpu.VMEM((shard_count, chunks, part, TOPK), f32),
            pltpu.VMEM((langs, MAIN, TOPK), f32),
            pltpu.VMEM((langs, TAIL, TOPK), f32),
            pltpu.VMEM((langs, MAIN, TOPK), f32),
            pltpu.VMEM((langs, TAIL, TOPK), f32),
            pltpu.VMEM((count, langs * MAIN), f32),
            pltpu.VMEM((count, langs * TAIL), f32),
            dma, *[dma((langs,))] * 4, *[dma((shard_count, langs))] * 4,
            *[dma((shard_count, chunks))] * 2, *[dma((langs,))] * 4,
        ],
        compiler_params=pltpu.CompilerParams(collective_id=0, has_side_effects=True),
    )(queries, routes.reshape(1, count), corpus)


def solution(mesh):
    placed = (P(("lang", "shard"), None), P(("lang", "shard"), None), P(("lang", "shard"), None))
    return jax.shard_map(
        shards, mesh=mesh, in_specs=placed, out_specs=P(("lang", "shard"), None), check_vma=False
    )
```
